32 devices in a mesh: dp: 4 (over x, y), ep: 8 (over z, core).
Axes of the slice: x: 2, y: 2, z: 4, core: 2. Of those that a mesh axis runs over, the one named last changes fastest.
Arguments:
- x_in: bfloat16 [131072, 320], P(('dp', 'ep')), parts along dimension 0
- d_out: bfloat16 [131072, 320], P(('dp', 'ep')), parts along dimension 0
- idx_a: int32 [131072, 1], P(('dp', 'ep')), parts along dimension 0
- gate_a: float32 [131072, 1], P(('dp', 'ep')), parts along dimension 0
- idx_b: int32 [131072, 1], P(('dp', 'ep')), parts along dimension 0
- gate_b: float32 [131072, 1], P(('dp', 'ep')), parts along dimension 0
- w1_a: bfloat16 [16, 320, 512], P('ep')
- w3_a: bfloat16 [16, 320, 512], P('ep')
- w2_a: bfloat16 [16, 512, 320], P('ep')
- ws1_a: bfloat16 [320, 512], replicated
- ws3_a: bfloat16 [320, 512], replicated
- ws2_a: bfloat16 [512, 320], replicated
- w1_b: bfloat16 [16, 320, 512], P('ep')
- w3_b: bfloat16 [16, 320, 512], P('ep')
- w2_b: bfloat16 [16, 512, 320], P('ep')
- ws1_b: bfloat16 [320, 512], replicated
- ws3_b: bfloat16 [320, 512], replicated
- ws2_b: bfloat16 [512, 320], replicated
Outputs:
- output 1: bfloat16 [131072, 320], P(('dp', 'ep')), parts along dimension 0
- output 2: bfloat16 [131072, 320], P(('dp', 'ep')), parts along dimension 0
- output 3: float32 [64, 320, 512], P(('dp', 'ep')), parts along dimension 0
- output 4: float32 [64, 320, 512], P(('dp', 'ep')), parts along dimension 0
- output 5: float32 [64, 512, 320], P(('dp', 'ep')), parts along dimension 0
- output 6: float32 [64, 320, 512], P(('dp', 'ep')), parts along dimension 0
- output 7: float32 [64, 320, 512], P(('dp', 'ep')), parts along dimension 0
- output 8: float32 [64, 512, 320], P(('dp', 'ep')), parts along dimension 0
- output 9: float32 [131072, 1], P(('dp', 'ep')), parts along dimension 0
- output 10: float32 [131072, 1], P(('dp', 'ep')), parts along dimension 0
There are 4 independent parts. The reference program is written for one: setup_inputs(seed, part) draws one part's arguments, and reference() takes and returns one part's arrays. A program takes and returns all parts, laid end to end along the dimension named above; an argument that names none is the same for every part.
All inputs are finite; a program needn't handle non-finite values.
Results may differ from the reference program's by a relative error of at most 0.00549.
Values are sent between devices in bfloat16 or wider.
A program may use at most 1 GiB of HBM per device.

```python
import jax
import jax.numpy as jnp
from jax import lax

D_MODEL = 320
FF_EXPERT = 512
FF_SHARED = 512
EXPERTS = 16
TOP_K = 1
TOKENS = 4096
GROUP_SIZE = 8
REP_COUNT = 512
CAPACITY = 512

PART_TOKENS = GROUP_SIZE * TOKENS
GROUP_ROWS = GROUP_SIZE * CAPACITY


def draw_routing(rng_key):
    fixed_ids = jnp.repeat(jnp.arange(TOP_K, dtype=jnp.int32), REP_COUNT)
    spare_ids = jnp.repeat(jnp.arange(TOP_K, EXPERTS, dtype=jnp.int32), REP_COUNT)

    def one_device(dev_key):
        sub_keys = jax.random.split(dev_key, 4)
        picked = jax.random.permutation(sub_keys[0], spare_ids)[: TOKENS - TOP_K * REP_COUNT]
        base_ids = jax.random.permutation(sub_keys[1], jnp.concatenate([fixed_ids, picked]))
        shift_by = jax.random.randint(sub_keys[2], (), 0, EXPERTS, dtype=jnp.int32)
        turn_by = jax.random.randint(sub_keys[3], (TOKENS, 1), 0, TOP_K, dtype=jnp.int32)
        offsets = (jnp.arange(TOP_K, dtype=jnp.int32)[None, :] + turn_by) % TOP_K
        return (base_ids[:, None] + offsets + shift_by) % EXPERTS

    dev_keys = jax.random.split(rng_key, GROUP_SIZE)
    return jax.vmap(one_device)(dev_keys).reshape(PART_TOKENS, TOP_K)


def normal_bf16(rng_key, out_shape, scale):
    return (jax.random.normal(rng_key, out_shape, jnp.float32) * scale).astype(jnp.bfloat16)


def layer_weights(weight_keys, key_start):
    return (
        normal_bf16(weight_keys[key_start], (EXPERTS, D_MODEL, FF_EXPERT), D_MODEL ** -0.5),
        normal_bf16(weight_keys[key_start + 1], (EXPERTS, D_MODEL, FF_EXPERT), D_MODEL ** -0.5),
        normal_bf16(weight_keys[key_start + 2], (EXPERTS, FF_EXPERT, D_MODEL), FF_EXPERT ** -0.5),
        normal_bf16(weight_keys[key_start + 3], (D_MODEL, FF_SHARED), D_MODEL ** -0.5),
        normal_bf16(weight_keys[key_start + 4], (D_MODEL, FF_SHARED), D_MODEL ** -0.5),
        normal_bf16(weight_keys[key_start + 5], (FF_SHARED, D_MODEL), FF_SHARED ** -0.5),
    )


def setup_inputs(seed: int = 0, part: int = 0) -> dict:
    part_keys = jax.random.split(jax.random.fold_in(jax.random.key(seed), part), 6)
    weight_keys = jax.random.split(jax.random.key(seed + 1), 12)
    gate_scale = TOP_K ** -0.5
    w1_a, w3_a, w2_a, ws1_a, ws3_a, ws2_a = layer_weights(weight_keys, 0)
    w1_b, w3_b, w2_b, ws1_b, ws3_b, ws2_b = layer_weights(weight_keys, 6)
    return {
        'x_in': normal_bf16(part_keys[0], (PART_TOKENS, D_MODEL), 1.0),
        'd_out': normal_bf16(part_keys[1], (PART_TOKENS, D_MODEL), 1.0),
        'idx_a': draw_routing(part_keys[2]),
        'gate_a': jax.random.uniform(part_keys[3], (PART_TOKENS, TOP_K), jnp.float32, 0.5, 1.5) * gate_scale,
        'idx_b': draw_routing(part_keys[4]),
        'gate_b': jax.random.uniform(part_keys[5], (PART_TOKENS, TOP_K), jnp.float32, 0.5, 1.5) * gate_scale,
        'w1_a': w1_a, 'w3_a': w3_a, 'w2_a': w2_a,
        'ws1_a': ws1_a, 'ws3_a': ws3_a, 'ws2_a': ws2_a,
        'w1_b': w1_b, 'w3_b': w3_b, 'w2_b': w2_b,
        'ws1_b': ws1_b, 'ws3_b': ws3_b, 'ws2_b': ws2_b,
    }


def route_tables(expert_ids):
    flat_ids = expert_ids.reshape(-1)
    pair_count = flat_ids.shape[0]
    pair_order = jnp.argsort(flat_ids, stable=True)
    expert_count = jax.ops.segment_sum(jnp.ones_like(flat_ids), flat_ids, num_segments=EXPERTS)
    expert_start = jnp.cumsum(expert_count) - expert_count
    position = flat_ids * GROUP_ROWS + jnp.argsort(pair_order) - expert_start[flat_ids]
    slot_index = jnp.arange(GROUP_ROWS)
    src_pair = pair_order[jnp.minimum(expert_start[:, None] + slot_index[None, :], pair_count - 1)]
    slot_used = slot_index[None, :] < expert_count[:, None]
    return src_pair, slot_used, position


def swiglu_hidden(rows, w_gate, w_up):
    pre_gate = jnp.dot(rows, w_gate, preferred_element_type=jnp.float32)
    pre_up = jnp.dot(rows, w_up, preferred_element_type=jnp.float32)
    return pre_gate, pre_up, (jax.nn.silu(pre_gate) * pre_up).astype(jnp.bfloat16)


def swiglu_grads(pre_gate, pre_up, d_hidden):
    sigma = jax.nn.sigmoid(pre_gate)
    d_gate = d_hidden * pre_up * sigma * (1.0 + pre_gate * (1.0 - sigma))
    d_up = d_hidden * pre_gate * sigma
    return d_gate.astype(jnp.bfloat16), d_up.astype(jnp.bfloat16)


def layer_forward(x_rows, expert_ids, gates, w_gate, w_up, w_down, s_gate, s_up, s_down):
    src_pair, slot_used, position = route_tables(expert_ids)
    sent = jnp.where(slot_used[:, :, None], x_rows[src_pair // TOP_K], 0)

    def one_expert(operands):
        rows, gate_w, up_w, down_w = operands
        hidden = swiglu_hidden(rows, gate_w, up_w)[2]
        return jnp.dot(hidden, down_w, preferred_element_type=jnp.float32).astype(jnp.bfloat16)

    expert_out = lax.map(one_expert, (sent, w_gate, w_up, w_down))
    per_pair = expert_out.reshape(-1, D_MODEL)[position].reshape(PART_TOKENS, TOP_K, D_MODEL)
    shared = jnp.dot(swiglu_hidden(x_rows, s_gate, s_up)[2], s_down, preferred_element_type=jnp.float32)
    mixed = x_rows.astype(jnp.float32) + shared + jnp.sum(gates[:, :, None] * per_pair.astype(jnp.float32), axis=1)
    return mixed.astype(jnp.bfloat16)


def layer_backward(x_rows, d_next, expert_ids, gates, w_gate, w_up, w_down, s_gate, s_up, s_down):
    src_pair, slot_used, position = route_tables(expert_ids)
    src_token = src_pair // TOP_K
    sent = jnp.where(slot_used[:, :, None], x_rows[src_token], 0)
    sent_dy = jnp.where(slot_used[:, :, None], d_next[src_token], 0)
    sent_gate = jnp.where(slot_used, gates.reshape(-1)[src_pair], 0.0)

    def one_expert(operands):
        rows, dy_part, gate_part, gate_w, up_w, down_w = operands
        pre_gate, pre_up, hidden = swiglu_hidden(rows, gate_w, up_w)
        projected = jnp.dot(dy_part, down_w.T, preferred_element_type=jnp.float32)
        gate_grad = jnp.sum(hidden.astype(jnp.float32) * projected, axis=1)
        scaled = (gate_part[:, None] * dy_part.astype(jnp.float32)).astype(jnp.bfloat16)
        dw_down = jnp.dot(hidden.T, scaled, preferred_element_type=jnp.float32)
        da_gate, da_up = swiglu_grads(pre_gate, pre_up, gate_part[:, None] * projected)
        dw_gate = jnp.dot(rows.T, da_gate, preferred_element_type=jnp.float32)
        dw_up = jnp.dot(rows.T, da_up, preferred_element_type=jnp.float32)
        d_rows = (jnp.dot(da_gate, gate_w.T, preferred_element_type=jnp.float32)
                  + jnp.dot(da_up, up_w.T, preferred_element_type=jnp.float32)).astype(jnp.bfloat16)
        return dw_gate, dw_up, dw_down, d_rows, gate_grad

    dw_gate, dw_up, dw_down, d_sent, gate_grad = lax.map(
        one_expert, (sent, sent_dy, sent_gate, w_gate, w_up, w_down))
    du_pair = d_sent.reshape(-1, D_MODEL)[position].reshape(PART_TOKENS, TOP_K, D_MODEL)
    d_gates = gate_grad.reshape(-1)[position].reshape(PART_TOKENS, TOP_K)
    s_pre = swiglu_hidden(x_rows, s_gate, s_up)
    s_projected = jnp.dot(d_next, s_down.T, preferred_element_type=jnp.float32)
    ds_gate, ds_up = swiglu_grads(s_pre[0], s_pre[1], s_projected)
    shared_dx = (jnp.dot(ds_gate, s_gate.T, preferred_element_type=jnp.float32)
                 + jnp.dot(ds_up, s_up.T, preferred_element_type=jnp.float32))
    d_x = d_next.astype(jnp.float32) + shared_dx + jnp.sum(du_pair.astype(jnp.float32), axis=1)
    return d_x.astype(jnp.bfloat16), dw_gate, dw_up, dw_down, d_gates


def reference(x_in, d_out, idx_a, gate_a, idx_b, gate_b,
              w1_a, w3_a, w2_a, ws1_a, ws3_a, ws2_a,
              w1_b, w3_b, w2_b, ws1_b, ws3_b, ws2_b):
    x_mid = layer_forward(x_in, idx_a, gate_a, w1_a, w3_a, w2_a, ws1_a, ws3_a, ws2_a)
    x_last = layer_forward(x_mid, idx_b, gate_b, w1_b, w3_b, w2_b, ws1_b, ws3_b, ws2_b)
    d_mid, dw1_b, dw3_b, dw2_b, dgate_b = layer_backward(
        x_mid, d_out, idx_b, gate_b, w1_b, w3_b, w2_b, ws1_b, ws3_b, ws2_b)
    d_first, dw1_a, dw3_a, dw2_a, dgate_a = layer_backward(
        x_in, d_mid, idx_a, gate_a, w1_a, w3_a, w2_a, ws1_a, ws3_a, ws2_a)
    return (x_last, d_first, dw1_a, dw3_a, dw2_a, dw1_b, dw3_b, dw2_b, dgate_a, dgate_b)
```

```python
import functools

import jax
import jax.numpy as jnp
from jax import lax
from jax.experimental import pallas as pl
from jax.experimental.pallas import tpu as pltpu
from jax.sharding import PartitionSpec as P

TILE = 256
LANES = 384
F32 = jnp.float32
BF16 = jnp.bfloat16


def slot_capacity(tokens, n_experts, top_k):
    return top_k * ((2 * tokens + n_experts - 1) // n_experts)


def mm(a, b):
    return jnp.dot(a, b, preferred_element_type=F32)


def mm_nt(a, b):
    return lax.dot_general(a, b, (((1,), (1,)), ((), ())), preferred_element_type=F32)


def mm_tn(a, b):
    return lax.dot_general(a, b, (((0,), (0,)), ((), ())), preferred_element_type=F32)


def row_to_column(row):
    return jnp.transpose(jnp.broadcast_to(row, (128, row.shape[1])))[:, :1]


def cost(flops, nbytes):
    return pl.CostEstimate(flops=int(flops), bytes_accessed=int(nbytes), transcendentals=0)


def tables_body(idx_ref, pos_ref, cnt_ref, *, n_experts, capacity):
    chunks = idx_ref.shape[1]
    earlier = (lax.broadcasted_iota(jnp.int32, (TILE, TILE), 0)
               < lax.broadcasted_iota(jnp.int32, (TILE, TILE), 1)).astype(F32).astype(BF16)
    expert = lax.broadcasted_iota(jnp.int32, (n_experts, TILE), 0)
    base = (lax.broadcasted_iota(jnp.int32, (n_experts, TILE), 0) * capacity).astype(F32)
    for layer in range(2):
        carry = jnp.zeros((n_experts, 1), F32)
        for c in range(chunks):
            hot = (expert == idx_ref[layer, c:c + 1, :]).astype(F32)
            before = mm(hot.astype(BF16), earlier)
            where = jnp.sum(hot * (before + carry + base), axis=0, keepdims=True)
            pos_ref[layer, c:c + 1, :] = where.astype(jnp.int32)
            carry = carry + jnp.sum(hot, axis=1, keepdims=True)
        cnt_ref[layer] = jnp.broadcast_to(carry, (n_experts, 128)).astype(jnp.int32)


def route_tables(idx_a, idx_b, n_experts, capacity):
    chunks = idx_a.size // TILE
    idx = jnp.stack([idx_a.reshape(chunks, TILE), idx_b.reshape(chunks, TILE)])
    pos, cnt = pl.pallas_call(
        functools.partial(tables_body, n_experts=n_experts, capacity=capacity),
        out_shape=(jax.ShapeDtypeStruct((2, chunks, TILE), jnp.int32),
                   jax.ShapeDtypeStruct((2, n_experts, 128), jnp.int32)),
        name="tables", cost_estimate=cost(3e8, 1e5))(idx)
    return pos.reshape(2, -1), cnt[:, :, 0]


def sort_body(pos_ref, x_ref, *refs, with_gate):
    if with_gate:
        gate_ref, out_ref, gout_ref, wide, slots = refs
    else:
        out_ref, wide, slots = refs
    tokens, width = x_ref.shape
    n_slots = out_ref.shape[0]

    @pl.loop(0, n_slots // TILE)
    def _(c):
        slots[pl.ds(c * TILE, TILE), :] = jnp.zeros((TILE, LANES), F32)

    @pl.loop(0, tokens // TILE)
    def _(c):
        at = pl.ds(c * TILE, TILE)
        wide[at, :width] = x_ref[at, :].astype(F32)
        if with_gate:
            wide[at, width:] = jnp.broadcast_to(row_to_column(gate_ref[pl.ds(c, 1), :]), (TILE, LANES - width))

    unroll = 32

    @pl.loop(0, tokens // unroll)
    def _(c):
        rows = [wide[pl.ds(c * unroll + i, 1), :] for i in range(unroll)]
        for i in range(unroll):
            slots[pl.ds(pos_ref[c * unroll + i], 1), :] = rows[i]

    @pl.loop(0, n_slots // TILE)
    def _(c):
        at = pl.ds(c * TILE, TILE)
        out_ref[at, :] = slots[at, :width].astype(BF16)
        if with_gate:
            gout_ref[pl.ds(c, 1), :] = jnp.transpose(slots[at, LANES - 128:])[127:128, :]


def sort_rows(pos, x, n_slots, gate=None):
    tokens, width = x.shape
    with_gate = gate is not None
    out_shape = [jax.ShapeDtypeStruct((n_slots, width), BF16)]
    args = [pos, x]
    if with_gate:
        args.append(gate)
        out_shape.append(jax.ShapeDtypeStruct((n_slots // TILE, TILE), F32))
    vmem = pl.BlockSpec(memory_space=pltpu.VMEM)
    return pl.pallas_call(
        functools.partial(sort_body, with_gate=with_gate),
        out_shape=out_shape,
        in_specs=[pl.BlockSpec(memory_space=pltpu.SMEM)] + [vmem] * (len(args) - 1),
        out_specs=[vmem] * len(out_shape),
        scratch_shapes=[pltpu.VMEM((tokens, LANES), F32), pltpu.VMEM((n_slots, LANES), F32)],
        name="sort_rows", cost_estimate=cost(2e9, 9e6))(*args)


def gather_rows(pos_ref, start, table, out):
    unroll = 16

    @pl.loop(0, TILE // unroll)
    def _(c):
        where = [pos_ref[start + c * unroll + i] for i in range(unroll)]
        rows = [table[pl.ds(p, 1), :] for p in where]
        for i in range(unroll):
            out[pl.ds(c * unroll + i, 1), :] = rows[i]


def expert_weights(w_ref):
    depth = w_ref.shape[0] * w_ref.shape[3]
    return tuple(w_ref[:, 0, m].reshape(depth, w_ref.shape[4]) for m in range(3))


def swiglu(a1, a3):
    sigma = jax.nn.sigmoid(a1)
    return sigma, (a1 * sigma * a3).astype(BF16)


def swiglu_grads(a1, a3, sigma, q):
    qs = q * sigma
    d1 = qs * a3 * (1.0 + a1 * (1.0 - sigma))
    return d1.astype(BF16), (qs * a1).astype(BF16)


def token_body(pos_ref, cnt_ref, *refs, fwd, bwd, n_experts, capacity):
    refs = list(refs)
    xs_ref = refs.pop(0)
    if bwd:
        dys_ref, gs_ref = refs.pop(0), refs.pop(0)
    w_ref, x_ref = refs.pop(0), refs.pop(0)
    if bwd:
        dy_ref = refs.pop(0)
    if fwd:
        g_ref = refs.pop(0)
    s1_ref, s3_ref, s2_ref = refs.pop(0), refs.pop(0), refs.pop(0)
    if fwd:
        y_ref = refs.pop(0)
    if bwd:
        dx_ref, dg_ref = refs.pop(0), refs.pop(0)
    if fwd:
        o_all, o_tmp = refs.pop(0), refs.pop(0)
    if bwd:
        du_all, du_tmp = refs.pop(0), refs.pop(0)
    step = pl.program_id(0)
    width = x_ref.shape[1]
    per = capacity // TILE

    for t in range(per):
        @pl.when(jnp.logical_and(step < n_experts, cnt_ref[jnp.minimum(step, n_experts - 1)] > t * TILE))
        def _():
            w1, w3, w2t = expert_weights(w_ref)
            rows = slice(t * TILE, (t + 1) * TILE)
            at = pl.ds(pl.multiple_of(step * capacity + t * TILE, TILE), TILE)
            u = xs_ref[0, rows, :]
            a1, a3 = mm(u, w1), mm(u, w3)
            sigma, h = swiglu(a1, a3)
            if fwd:
                o_all[at, :width] = mm_nt(h, w2t).astype(BF16).astype(F32)
            if bwd:
                p = mm(dys_ref[0, rows, :], w2t)
                dgate = jnp.sum(h.astype(F32) * p, axis=1, keepdims=True)
                g = row_to_column(gs_ref[pl.ds(step * per + t, 1), :])
                d1, d3 = swiglu_grads(a1, a3, sigma, g * p)
                du_all[at, :width] = (mm_nt(d1, w1) + mm_nt(d3, w3)).astype(BF16).astype(F32)
                du_all[at, width:] = jnp.broadcast_to(dgate, (TILE, LANES - width))

    @pl.when(step >= n_experts)
    def _():
        tile = step - n_experts
        start = tile * TILE
        if fwd:
            gather_rows(pos_ref, start, o_all, o_tmp)
        if bwd:
            gather_rows(pos_ref, start, du_all, du_tmp)
        x = x_ref[...]
        a1, a3 = mm(x, s1_ref[...]), mm(x, s3_ref[...])
        sigma, h = swiglu(a1, a3)
        if fwd:
            shared = mm(h, s2_ref[...])
            g = row_to_column(g_ref[pl.ds(tile, 1), :])
            y_ref[...] = (x.astype(F32) + shared + g * o_tmp[:, :width]).astype(BF16)
        if bwd:
            dy = dy_ref[...]
            p = mm_nt(dy, s2_ref[...])
            d1, d3 = swiglu_grads(a1, a3, sigma, p)
            dxs = mm_nt(d1, s1_ref[...]) + mm_nt(d3, s3_ref[...])
            dx_ref[...] = (dy.astype(F32) + dxs + du_tmp[:, :width]).astype(BF16)
            dg_ref[pl.ds(tile, 1), :] = jnp.transpose(du_tmp[:, LANES - 128:])[127:128, :]


def token_layer(pos, cnt, xs, weights, x, shared, capacity, gate=None, dys=None, gs=None, dy=None):
    fwd, bwd = gate is not None, dys is not None
    tokens, width = x.shape
    n_experts = cnt.shape[0]
    s1, s3, s2 = shared
    last = n_experts - 1
    expert_map = lambda i, *_: (jnp.minimum(i, last), 0, 0)
    token_map = lambda i, *_: (jnp.maximum(i - n_experts, 0), 0)
    whole = lambda a: pl.BlockSpec(a.shape, lambda i, *_: (0,) * a.ndim)
    rows = pl.BlockSpec((1, capacity, width), expert_map)
    toks = pl.BlockSpec((TILE, width), token_map)
    q, _, m, qd, ff = weights.shape
    wspec = pl.BlockSpec((q, 1, m, qd, ff), lambda i, *_: (0, jnp.minimum(i, last), 0, 0, 0))
    args, specs, outs, ospecs, scratch = [], [], [], [], []

    def add(a, s):
        args.append(a)
        specs.append(s)

    add(xs.reshape(n_experts, capacity, width), rows)
    if bwd:
        add(dys.reshape(n_experts, capacity, width), rows)
        add(gs, whole(gs))
    add(weights, wspec)
    add(x, toks)
    if bwd:
        add(dy, toks)
    if fwd:
        add(gate, whole(gate))
    for s in (s1, s3, s2):
        add(s, whole(s))
    slots = n_experts * capacity
    if fwd:
        outs.append(jax.ShapeDtypeStruct((tokens, width), BF16))
        ospecs.append(toks)
        scratch += [pltpu.VMEM((slots, LANES), F32), pltpu.VMEM((TILE, LANES), F32)]
    if bwd:
        outs += [jax.ShapeDtypeStruct((tokens, width), BF16), jax.ShapeDtypeStruct((tokens // TILE, TILE), F32)]
        ospecs += [toks, pl.BlockSpec((tokens // TILE, TILE), lambda i, *_: (0, 0))]
        scratch += [pltpu.VMEM((slots, LANES), F32), pltpu.VMEM((TILE, LANES), F32)]
    n_mm = (3 if fwd else 2) + (3 if bwd else 0)
    return pl.pallas_call(
        functools.partial(token_body, fwd=fwd, bwd=bwd, n_experts=n_experts, capacity=capacity),
        out_shape=outs,
        grid_spec=pltpu.PrefetchScalarGridSpec(
            num_scalar_prefetch=2, grid=(n_experts + tokens // TILE,),
            in_specs=specs, out_specs=ospecs, scratch_shapes=scratch),
        name="token_layer",
        cost_estimate=cost(2 * n_mm * 2 * tokens * width * ff, 3e7))(pos, cnt, *args)


def wgrad_body(cnt_ref, x_ref, dy_ref, g_ref, w1_ref, w3_ref, w2_ref, dw1_ref, dw3_ref, dw2_ref):
    e, src = pl.program_id(0), pl.program_id(1)
    per = x_ref.shape[2] // TILE

    @pl.when(src == 0)
    def _():
        dw1_ref[...] = jnp.zeros_like(dw1_ref)
        dw3_ref[...] = jnp.zeros_like(dw3_ref)
        dw2_ref[...] = jnp.zeros_like(dw2_ref)

    for t in range(per):
        @pl.when(cnt_ref[src, e] > t * TILE)
        def _():
            rows = slice(t * TILE, (t + 1) * TILE)
            u, dy = x_ref[0, 0, rows, :], dy_ref[0, 0, rows, :]
            g = row_to_column(g_ref[src, pl.ds(e * per + t, 1), :])
            a1, a3 = mm(u, w1_ref[0]), mm(u, w3_ref[0])
            sigma, h = swiglu(a1, a3)
            p = mm_nt(dy, w2_ref[0])
            scaled = (g * dy.astype(F32)).astype(BF16)
            dw2_ref[0] += mm_tn(h, scaled)
            d1, d3 = swiglu_grads(a1, a3, sigma, g * p)
            dw1_ref[0] += mm_tn(u, d1)
            dw3_ref[0] += mm_tn(u, d3)


def weight_grads(x_rows, dy_rows, gates, w1, w3, w2, capacity):
    n_local, width, ff = w1.shape
    group = x_rows.shape[0]
    counts = jnp.sum(gates.reshape(group, n_local, capacity) > 0.0, axis=2, dtype=jnp.int32)
    shape = (group, n_local, capacity, width)
    rows = pl.BlockSpec((1, 1, capacity, width), lambda e, s, *_: (s, e, 0, 0))
    mat = lambda a: pl.BlockSpec((1,) + a.shape[1:], lambda e, s, *_: (e, 0, 0))
    grads = [jax.ShapeDtypeStruct(a.shape, F32) for a in (w1, w3, w2)]
    return pl.pallas_call(
        wgrad_body,
        out_shape=grads,
        grid_spec=pltpu.PrefetchScalarGridSpec(
            num_scalar_prefetch=1, grid=(n_local, group),
            in_specs=[rows, rows, pl.BlockSpec(gates.shape, lambda e, s, *_: (0, 0, 0)),
                      mat(w1), mat(w3), mat(w2)],
            out_specs=[mat(w1), mat(w3), mat(w2)]),
        name="weight_grads",
        cost_estimate=cost(6 * 2 * group * n_local * capacity * width * ff, 2e7),
    )(counts, x_rows.reshape(shape), dy_rows.reshape(shape), gates, w1, w3, w2)


def exchange(rows, group_size):
    shaped = rows.reshape((group_size, rows.shape[0] // group_size) + rows.shape[1:])
    return lax.all_to_all(shaped, 'ep', 0, 0, tiled=True)


def gather_weights(w1, w3, w2, replicas):
    quarter = w1.shape[1] // replicas
    at = lax.axis_index('dp') * quarter
    part = jnp.stack([lax.dynamic_slice_in_dim(w1, at, quarter, 1),
                      lax.dynamic_slice_in_dim(w3, at, quarter, 1),
                      jnp.swapaxes(lax.dynamic_slice_in_dim(w2, at, quarter, 2), 1, 2)], axis=1)
    whole = lax.all_gather(part, ('dp', 'ep'), axis=0, tiled=True)
    return whole.reshape((replicas, -1) + whole.shape[1:])


def solution(mesh):
    group_size = mesh.shape['ep']
    replicas = mesh.shape['dp']
    token_spec = P(('dp', 'ep'), None)
    expert_spec = P('ep', None, None)
    shared_spec = P(None, None)
    grad_spec = P(('dp', 'ep'), None, None)
    layer_specs = (expert_spec,) * 3 + (shared_spec,) * 3

    def device_step(x_in, d_out, idx_a, gate_a, idx_b, gate_b,
                    w1_a, w3_a, w2_a, ws1_a, ws3_a, ws2_a,
                    w1_b, w3_b, w2_b, ws1_b, ws3_b, ws2_b):
        shared_a, shared_b = (ws1_a, ws3_a, ws2_a), (ws1_b, ws3_b, ws2_b)
        tokens, top_k = idx_a.shape
        n_experts = w1_a.shape[0] * group_size
        capacity = slot_capacity(tokens, n_experts, top_k)
        n_slots = n_experts * capacity
        gate_a, gate_b = gate_a.reshape(-1, TILE), gate_b.reshape(-1, TILE)
        all_a = gather_weights(w1_a, w3_a, w2_a, replicas)
        pos, cnt = route_tables(idx_a, idx_b, n_experts, capacity)
        pos_a, pos_b, cnt_a, cnt_b = pos[0], pos[1], cnt[0], cnt[1]
        dys_b, gs_b = sort_rows(pos_b, d_out, n_slots, gate_b)
        dy_rows_b, g_rows_b = exchange(dys_b, group_size), exchange(gs_b, group_size)
        xs_a, = sort_rows(pos_a, x_in, n_slots)
        x_rows_a = exchange(xs_a, group_size)
        x_mid, = token_layer(pos_a, cnt_a, xs_a, all_a, x_in, shared_a, capacity, gate=gate_a)
        all_b = gather_weights(w1_b, w3_b, w2_b, replicas)
        xs_b, = sort_rows(pos_b, x_mid, n_slots)
        x_rows_b = exchange(xs_b, group_size)
        x_last, d_mid, dgate_b = token_layer(pos_b, cnt_b, xs_b, all_b, x_mid, shared_b, capacity,
                                             gate=gate_b, dys=dys_b, gs=gs_b, dy=d_out)
        w1_r, w3_r, w2_r, x_again, _ = lax.optimization_barrier((w1_a, w3_a, w2_a, x_in, x_mid))
        all_a2 = gather_weights(w1_r, w3_r, w2_r, replicas)
        dys_a, gs_a = sort_rows(pos_a, d_mid, n_slots, gate_a)
        dy_rows_a, g_rows_a = exchange(dys_a, group_size), exchange(gs_a, group_size)
        xs_a2, = sort_rows(pos_a, x_again, n_slots)
        d_first, dgate_a = token_layer(pos_a, cnt_a, xs_a2, all_a2, x_again, shared_a, capacity,
                                       dys=dys_a, gs=gs_a, dy=d_mid)
        dw1_b, dw3_b, dw2_b = weight_grads(x_rows_b, dy_rows_b, g_rows_b, w1_b, w3_b, w2_b, capacity)
        dw1_a, dw3_a, dw2_a = weight_grads(x_rows_a, dy_rows_a, g_rows_a, w1_a, w3_a, w2_a, capacity)
        return (x_last, d_first, dw1_a, dw3_a, dw2_a, dw1_b, dw3_b, dw2_b,
                dgate_a.reshape(tokens, top_k), dgate_b.reshape(tokens, top_k))

    in_specs = (token_spec,) * 6 + layer_specs + layer_specs
    out_specs = (token_spec, token_spec) + (grad_spec,) * 6 + (token_spec, token_spec)
    return jax.shard_map(device_step, mesh=mesh, in_specs=in_specs, out_specs=out_specs, check_vma=False)
```
